32 devices in a mesh: dp: 4 (over y, x), expert: 8 (over z, core).
Axes of the slice: x: 2, y: 2, z: 4, core: 2. Of those that a mesh axis runs over, the one named last changes fastest.
Arguments:
- grad_out: bfloat16 [4096, 3072], P(('dp', 'expert')), may hold values from -6 to 6
- expert_ids: int32 [4096, 2], P(('dp', 'expert')), may hold values from 0 to 7, all different within a row; in each aligned block of 128 rows (0 to 127, 128 to 255, ...) at most 36 rows name the same one
- down_weight: bfloat16 [8, 1024, 3072], P('expert'), may hold values from -0.109375 to 0.109375
- history_grad: float32 [8, 8], replicated, may hold values from 0.5 to 3
- history_hidden: float32 [8, 8], replicated, may hold values from 0.5 to 3
Outputs:
- hidden_scaled: bfloat16 [4, 8, 288, 1024], P('dp', 'expert')
- new_history_grad: float32 [8, 8], replicated
- new_history_hidden: float32 [8, 8], replicated
The draws below stay inside these ranges and needn't reach their ends.
Inputs may be any that keep to these rules, and one draw needn't show every extreme that they name: `expert_ids`: each row names 2 different experts; among the 128 rows of one device no expert is named more than 36 times, a bound that some block reaches in some devices.
All inputs are finite; a program needn't handle non-finite values.
Results may differ from the reference program's by a relative error of at most 0.0045.
Values may be sent and summed in bfloat16 or wider, within the bound.
A program may use at most 128 MiB of HBM per device.

```python
import math
import jax
import jax.numpy as jnp
import numpy as np
from jax import lax

D = 3072
EXPERTS = 8
TOP = 2
FF_DEV = 1024
HIST = 8
TOK_DEV = 128
CAP = 36
TOKENS = 4096
N_DP = 4
N_EXPERT = 8


def steps_of(key, dims, split, smallest, top_value):
    level, own = 1.0, jax.random.fold_in(key, 6)
    for axis_at, shards_of in split:
        steps = jnp.exp(jax.random.uniform(jax.random.fold_in(own, axis_at), (shards_of,), jnp.float32, smallest / len(split), top_value / len(split)))
        level = level * jnp.repeat(steps, dims[axis_at] // shards_of).reshape([-1 if axis == axis_at else 1 for axis in range(len(dims))])
    return level


def deal_out(own_key, own, number, rows, number_of, top, bound, lean):
    ranking = jax.random.permutation(own_key, number_of)
    packed, ordinary = portions_of(number_of, rows * top, bound, lean, True), portions_of(number_of, rows * top, bound, lean, False)
    places = jnp.arange(number_of)

    def named(lengths, turn):
        used = int((lengths > 0).sum())
        fixed = max(1, used // 4)
        moved = fixed + (places - fixed + turn * (used - fixed)) % max(1, number_of - fixed)
        return jnp.zeros((number_of,), jnp.int32).at[ranking[jnp.where(places < fixed, places, moved)]].set(jnp.asarray(lengths, jnp.int32))

    lengths = jnp.where(number % 4 == 0, named(packed, number // 4), named(ordinary, number - number // 4 - 1))
    mixed = jax.random.permutation(jax.random.fold_in(own, 3), number_of)
    giver, receiver = mixed[0:number_of // 2 * 2:2], mixed[1:number_of // 2 * 2:2]
    room = jnp.minimum(lengths[giver] - 1, bound - lengths[receiver]) // 2
    room = jnp.where((giver == ranking[0]) | (receiver == ranking[0]) | (lengths[receiver] == 0), 0, jnp.maximum(room, 0))
    moved = jax.random.randint(jax.random.fold_in(own, 4), (number_of // 2,), 0, 1 << 20) % (room + 1)
    lengths = lengths.at[giver].add(-moved).at[receiver].add(moved)
    items = jnp.searchsorted(jnp.cumsum(lengths), jnp.arange(rows * top), side="right").astype(jnp.int32)
    grid = items.reshape(top, rows).T
    grid = grid[jax.random.permutation(jax.random.fold_in(own, 1), rows)]
    turn = jax.random.randint(jax.random.fold_in(own, 2), (rows, 1), 0, top)
    return jnp.take_along_axis(grid, (jnp.arange(top)[None, :] + turn) % top, axis=1)


def portions_of(count, total, bound, slope, full):
    loads = [(1 << 20) // math.isqrt(rank ** slope) + 1 for rank in range(1, count + 1)]
    largest = bound if full else min(bound, max(-(-total // count), total * loads[0] // sum(loads)))
    least = 1 if total - largest >= count - 1 else 0
    given, surplus = [largest] + [least] * (count - 1), total - largest - least * (count - 1)
    while surplus > 0:
        candidates = [i for i in range(1, count) if given[i] < largest] or [i for i in range(1, count) if given[i] < bound]
        mass, budget = sum([loads[i] for i in candidates]), surplus
        for i in candidates:
            extra = min(bound - given[i], max(1, budget * loads[i] // mass), surplus)
            given[i] = given[i] + extra
            surplus = surplus - extra
    return np.array(given)


def centred(own_key, shape, spread, bound, split=(), held_as=jnp.bfloat16):
    result = jax.random.normal(own_key, shape, jnp.float32) * spread
    if len(split) > 0:
        result = steps_of(own_key, shape, split, -0.22, 0.18) * result
    return jnp.clip(result, min=-bound, max=bound).astype(held_as)


def setup_inputs(seed: int = 0) -> dict:
    seeds = jax.random.split(jax.random.key(seed), 6)
    grad_out = centred(seeds[0], (TOKENS, D), 1.0, 6.0, ((0, 32),))
    expert_ids_keys = jax.random.split(jax.random.fold_in(seeds[1], 1), TOKENS // TOK_DEV)
    expert_ids_turns = jax.random.permutation(jax.random.fold_in(seeds[1], 3), TOKENS // TOK_DEV)
    expert_ids = jax.vmap(lambda own, number: deal_out(jax.random.fold_in(seeds[1], 2), own, number, TOK_DEV, EXPERTS, TOP, CAP, 2))(expert_ids_keys, expert_ids_turns).reshape((TOKENS, TOP))
    down_weight = centred(seeds[2], (N_EXPERT, FF_DEV, D), D ** -0.5, 0.109375, ((0, 8),))
    history_grad = jnp.clip(jnp.exp(jax.random.uniform(seeds[3], (HIST, EXPERTS), jnp.float32, math.log(0.5), math.log(3.0))), 0.5, 3.0)
    history_hidden = jnp.clip(jnp.exp(jax.random.uniform(seeds[4], (HIST, EXPERTS), jnp.float32, math.log(0.5), math.log(3.0))), 0.5, 3.0)
    return {"grad_out": grad_out, "expert_ids": expert_ids, "down_weight": down_weight, "history_grad": history_grad, "history_hidden": history_hidden}


def reference(grad_out, expert_ids, down_weight, history_grad, history_hidden):
    slices = N_EXPERT // EXPERTS
    routing = expert_ids.reshape(N_DP, N_EXPERT, TOK_DEV * TOP)
    onehot = (routing[..., None] == jnp.arange(EXPERTS, dtype=jnp.int32)).astype(jnp.int32)
    before = jnp.cumsum(onehot, axis=2) - onehot
    slot_index = jnp.sum(before * onehot, axis=-1).astype(jnp.int32)
    scale_in = 1.0 / jnp.max(history_grad, axis=0)
    scale_hidden = 1.0 / jnp.max(history_hidden, axis=0)
    gradients = grad_out.reshape(N_DP, N_EXPERT, TOK_DEV, D)
    row_peak = jnp.max(jnp.abs(gradients.astype(jnp.float32)), axis=-1)
    routed = jnp.max(onehot.reshape(N_DP, N_EXPERT, TOK_DEV, TOP, EXPERTS), axis=3) > 0
    grad_amax = jnp.max(jnp.where(routed, row_peak[..., None], 0.0), axis=(0, 1, 2))
    token_of = jnp.arange(TOK_DEV * TOP, dtype=jnp.int32) // TOP
    weights = down_weight.reshape(EXPERTS, slices * FF_DEV, D)
    source_index = jnp.broadcast_to(jnp.arange(N_EXPERT, dtype=jnp.int32)[:, None], (N_EXPERT, TOK_DEV * TOP))

    def one_replica(inputs):
        grads_here, routing_here, slots_here = inputs
        token_rows = grads_here[:, token_of].astype(jnp.float32)
        quantized = jnp.clip(token_rows * scale_in[routing_here][..., None], -1.0, 1.0).astype(jnp.bfloat16)
        buffer = jnp.zeros((EXPERTS, N_EXPERT, CAP, D), jnp.bfloat16)
        buffer = buffer.at[routing_here, source_index, slots_here].set(quantized)

        def one_expert(pair):
            expert, block = pair
            received = block.reshape(N_EXPERT * CAP, D)
            product = jnp.dot(received, weights[expert].T, preferred_element_type=jnp.float32)
            hidden = product / scale_in[expert]
            scaled = jnp.clip(hidden * scale_hidden[expert], -1.0, 1.0).astype(jnp.bfloat16)
            scaled = scaled.reshape(N_EXPERT * CAP, slices, FF_DEV).transpose(1, 0, 2)
            return scaled, jnp.max(jnp.abs(hidden))

        scaled, peak_values = lax.map(one_expert, (jnp.arange(EXPERTS, dtype=jnp.int32), buffer))
        return scaled.reshape(N_EXPERT, N_EXPERT * CAP, FF_DEV), peak_values

    hidden_scaled, peak_values = lax.map(one_replica, (gradients, routing, slot_index))
    hidden_amax = jnp.max(peak_values, axis=0)
    new_history_grad = jnp.concatenate([history_grad[1:], grad_amax[None, :]], axis=0)
    new_history_hidden = jnp.concatenate([history_hidden[1:], hidden_amax[None, :]], axis=0)
    return hidden_scaled, new_history_grad, new_history_hidden
```

```python
import functools

import jax
import jax.numpy as jnp
from jax import lax
from jax.experimental import pallas as pl
from jax.experimental.pallas import tpu as pltpu
from jax.sharding import PartitionSpec as P

MESH = pl.DeviceIdType.MESH
LANES = 128


def flip_bits(q, k, count):
    out, bit = 0, 1
    while bit < count:
        a, b = (q // bit) % 2, (k // bit) % 2
        out = out + bit * (a + b - 2 * a * b)
        bit *= 2
    return out


def kernel(
    n_dp, n_exp, experts, capacity,
    grad_ref, ids_ref, hist_g_ref, hist_h_ref, weight_hbm,
    out_ref, new_g_ref, new_h_ref,
    weight, send, recv, slots, mine, folded, dp_in, ex_in,
    weight_sem, send_sem, recv_sem, dps_sem, dpr_sem, exs_sem, exr_sem,
):
    tokens = grad_ref.shape[0]
    slices = n_exp // experts
    chips = n_exp // 2
    my_dp, me = lax.axis_index("dp"), lax.axis_index("expert")
    q0, c0 = me // 2, me % 2
    partner = q0 * 2 + 1 - c0
    own = me // slices
    load = pltpu.make_async_copy(weight_hbm.at[0], weight, weight_sem)
    load.start()

    barrier = pltpu.get_barrier_semaphore()

    def greet_exp(j, x):
        pl.semaphore_signal(barrier, inc=1, device_id=(my_dp, (me + j) % n_exp), device_id_type=MESH)
        return x

    def greet_dp(j, x):
        pl.semaphore_signal(barrier, inc=1, device_id=((my_dp + j) % n_dp, me), device_id_type=MESH)
        return x

    lax.fori_loop(1, n_exp, greet_exp, 0)
    lax.fori_loop(1, n_dp, greet_dp, 0)

    lane = lax.broadcasted_iota(jnp.int32, (tokens, LANES), 1)
    ids = ids_ref[...]
    routed = (ids[:, 0:1] == lane) | (ids[:, 1:2] == lane)
    mask_t = jnp.where(routed, 1.0, 0.0).T
    row = lax.broadcasted_iota(jnp.int32, (tokens, tokens), 0)
    col = lax.broadcasted_iota(jnp.int32, (tokens, tokens), 1)
    earlier = jnp.where(row < col, 1.0, 0.0).astype(jnp.bfloat16)
    before = jnp.dot(mask_t.astype(jnp.bfloat16), earlier, preferred_element_type=jnp.float32)
    slots[...] = jnp.where(mask_t > 0.5, before, -1.0)
    scale_in = 1.0 / jnp.max(hist_g_ref[...], axis=0, keepdims=True)
    scale_hidden = 1.0 / jnp.max(hist_h_ref[...], axis=0, keepdims=True)
    which = lax.broadcasted_iota(jnp.int32, (1, experts), 1)

    def pick(values, e):
        return jnp.sum(jnp.where(which == e, values, 0.0), axis=1, keepdims=True)

    position = lax.broadcasted_iota(jnp.int32, (capacity, tokens), 0).astype(jnp.float32)

    def prepare(e):
        onehot = jnp.where(slots[pl.ds(e, 1), :] == position, 1.0, 0.0).astype(jnp.bfloat16)
        rows = jnp.dot(onehot, grad_ref[...], preferred_element_type=jnp.float32)
        send[e] = jnp.clip(rows * pick(scale_in, e), -1.0, 1.0).astype(jnp.bfloat16)

    def outgoing(d):
        return pltpu.make_async_remote_copy(
            src_ref=send.at[d // slices], dst_ref=recv.at[me],
            send_sem=send_sem.at[d], recv_sem=recv_sem.at[me],
            device_id=(my_dp, d), device_id_type=MESH,
        )

    def incoming(s):
        return pltpu.make_async_remote_copy(
            src_ref=send.at[0], dst_ref=recv.at[s],
            send_sem=send_sem.at[s], recv_sem=recv_sem.at[s],
            device_id=(my_dp, s), device_id_type=MESH,
        )

    def chip_of(j):
        k = jnp.where(j < 2, j, chips + 1 - j)
        if chips & (chips - 1) == 0:
            return flip_bits(q0, k, chips)
        return (q0 + k) % chips

    def source_of(j):
        if chips & (chips - 1) == 0:
            return chip_of(j)
        k = jnp.where(j < 2, j, chips + 1 - j)
        return (q0 + chips - k) % chips

    def prepare_pair(q):
        prepare(2 * q + c0)
        prepare(2 * q + 1 - c0)

    def send_pair(q):
        outgoing(2 * q + c0).start()
        outgoing(2 * q + 1 - c0).start()

    greeted = n_exp + n_dp - 2
    if slices == 1:
        prepare_pair(chip_of(jnp.int32(1)))
        pl.semaphore_wait(barrier, greeted)

        def step(j, x):
            prepare_pair(chip_of((j + 1) % chips))
            send_pair(chip_of(j))
            return x
    else:
        def fill(e, x):
            prepare(e)
            return x

        lax.fori_loop(0, experts, fill, 0)
        pl.semaphore_wait(barrier, greeted)

        def step(j, x):
            send_pair(chip_of(j))
            return x

    lax.fori_loop(1, chips, step, 0)
    outgoing(partner).start()

    row_peak = jnp.max(jnp.abs(grad_ref[...]).astype(jnp.float32), axis=1, keepdims=True)
    grad_peak = jnp.max(jnp.where(routed, row_peak, 0.0), axis=0, keepdims=True)

    back = 1.0 / pick(scale_in, own)
    own_hidden = pick(scale_hidden, own)
    load.wait()

    def multiply(block, s):
        product = lax.dot_general(
            block, weight[...], (((1,), (1,)), ((), ())), preferred_element_type=jnp.float32
        )
        hidden = product * back
        out_ref[s] = jnp.clip(hidden * own_hidden, -1.0, 1.0).astype(jnp.bfloat16)
        return jnp.max(jnp.max(jnp.abs(hidden), axis=0, keepdims=True), axis=1, keepdims=True)

    peak = multiply(send[own], me)

    def take(s, peak):
        incoming(s).wait_recv()
        return jnp.maximum(peak, multiply(recv[s], s))

    def take_step(i, peak):
        q = source_of(i // 2)
        c = (c0 + i % 2) % 2
        return take(2 * q + c, peak)

    peak = take(partner, peak)
    peak = lax.fori_loop(2, n_exp, take_step, peak)

    at = lax.broadcasted_iota(jnp.int32, (1, LANES), 1)
    hidden_peak = jnp.where(at == own, peak, 0.0)
    part = lax.broadcasted_iota(jnp.int32, (8, LANES), 0)
    mine[...] = jnp.where(part == 0, grad_peak, jnp.where(part == 1, hidden_peak, 0.0))

    def dp_copy(j, back_way):
        peer = (my_dp + (n_dp - j if back_way else j)) % n_dp
        slot = peer if back_way else my_dp
        return pltpu.make_async_remote_copy(
            src_ref=mine, dst_ref=dp_in.at[slot], send_sem=dps_sem.at[j], recv_sem=dpr_sem.at[slot],
            device_id=(peer, me), device_id_type=MESH,
        )

    def ex_copy(j, back_way):
        peer = (me + (n_exp - j if back_way else j)) % n_exp
        slot = peer if back_way else me
        return pltpu.make_async_remote_copy(
            src_ref=folded, dst_ref=ex_in.at[slot], send_sem=exs_sem.at[j], recv_sem=exr_sem.at[slot],
            device_id=(my_dp, peer), device_id_type=MESH,
        )

    for copy, count, source, target, buffer in (
        (dp_copy, n_dp, mine, folded, dp_in), (ex_copy, n_exp, folded, mine, ex_in)
    ):
        def start(j, x, copy=copy):
            copy(j, False).start()
            return x

        def fold(j, best, copy=copy, count=count, buffer=buffer):
            copy(j, True).wait_recv()
            at_slot = ((my_dp if copy is dp_copy else me) + count - j) % count
            return jnp.maximum(best, buffer[at_slot])

        def finish(j, x, copy=copy):
            copy(j, False).wait_send()
            return x

        lax.fori_loop(1, count, start, 0)
        best = lax.fori_loop(1, count, fold, source[...])
        lax.fori_loop(1, count, finish, 0)
        target[...] = best

    keep = hist_g_ref.shape[0] - 1
    new_g_ref[0:keep, :] = hist_g_ref[1:keep + 1, :]
    new_g_ref[keep:keep + 1, :] = best[0:1, 0:experts]
    new_h_ref[0:keep, :] = hist_h_ref[1:keep + 1, :]
    new_h_ref[keep:keep + 1, :] = best[1:2, 0:experts]

    def drain(j, x):
        outgoing((me + j) % n_exp).wait_send()
        return x

    lax.fori_loop(1, n_exp, drain, 0)


def per_device(grad_out, expert_ids, down_weight, history_grad, history_hidden):
    tokens, width = grad_out.shape
    experts = history_grad.shape[1]
    n_dp, n_exp = lax.axis_size("dp"), lax.axis_size("expert")
    capacity = tokens * 9 // 32
    units = down_weight.shape[1]
    vmem = pl.BlockSpec(memory_space=pltpu.VMEM)
    dma = pltpu.SemaphoreType.DMA
    out, new_g, new_h = pl.pallas_call(
        functools.partial(kernel, n_dp, n_exp, experts, capacity),
        out_shape=(
            jax.ShapeDtypeStruct((n_exp, capacity, units), jnp.bfloat16),
            jax.ShapeDtypeStruct(history_grad.shape, jnp.float32),
            jax.ShapeDtypeStruct(history_hidden.shape, jnp.float32),
        ),
        in_specs=[vmem, vmem, vmem, vmem, pl.BlockSpec(memory_space=pl.ANY)],
        out_specs=(vmem, vmem, vmem),
        scratch_shapes=[
            pltpu.VMEM((units, width), jnp.bfloat16),
            pltpu.VMEM((experts, capacity, width), jnp.bfloat16),
            pltpu.VMEM((n_exp, capacity, width), jnp.bfloat16),
            pltpu.VMEM((LANES, tokens), jnp.float32),
            pltpu.VMEM((8, LANES), jnp.float32),
            pltpu.VMEM((8, LANES), jnp.float32),
            pltpu.VMEM((n_dp, 8, LANES), jnp.float32),
            pltpu.VMEM((n_exp, 8, LANES), jnp.float32),
            dma, dma((n_exp,)), dma((n_exp,)), dma((n_dp,)), dma((n_dp,)), dma((n_exp,)), dma((n_exp,)),
        ],
        compiler_params=pltpu.CompilerParams(
            collective_id=0, has_side_effects=True, vmem_limit_bytes=60 * 1024 * 1024
        ),
    )(grad_out, expert_ids, history_grad, history_hidden, down_weight)
    return out.reshape(1, 1, n_exp * capacity, units), new_g, new_h


def solution(mesh):
    in_specs = (
        P(("dp", "expert"), None),
        P(("dp", "expert"), None),
        P("expert", None, None),
        P(),
        P(),
    )
    out_specs = (P("dp", "expert", None, None), P(), P())
    return jax.shard_map(
        per_device, mesh=mesh, in_specs=in_specs, out_specs=out_specs, check_vma=False
    )
```

```python
import functools

import jax
import jax.numpy as jnp
from jax import lax
from jax.experimental import pallas as pl
from jax.experimental.pallas import tpu as pltpu
from jax.sharding import PartitionSpec as P

MESH = pl.DeviceIdType.MESH
LANES = 128


def flip_bits(q, k, count):
    out, bit = 0, 1
    while bit < count:
        a, b = (q // bit) % 2, (k // bit) % 2
        out = out + bit * (a + b - 2 * a * b)
        bit *= 2
    return out


def kernel(
    n_dp, n_exp, experts, capacity,
    grad_ref, ids_ref, hist_g_ref, hist_h_ref, weight_hbm,
    out_ref, new_g_ref, new_h_ref,
    weight, send, send_rest, recv, recv_rest, rest_rows, slots, mine, peaks_in,
    weight_sem, send_sem, recv_sem, send_rest_sem, recv_rest_sem, peak_send_sem, peak_recv_sem,
):
    tokens = grad_ref.shape[0]
    main = send.shape[1]
    slices = n_exp // experts
    chips = n_exp // 2
    my_dp, me = lax.axis_index("dp"), lax.axis_index("expert")
    q0, c0 = me // 2, me % 2
    partner = q0 * 2 + 1 - c0
    own = me // slices
    load = pltpu.make_async_copy(weight_hbm.at[0], weight, weight_sem)
    load.start()

    barrier = pltpu.get_barrier_semaphore()

    everyone = n_dp * n_exp
    here = my_dp * n_exp + me

    def greet(j, x):
        peer = (here + j) % everyone
        pl.semaphore_signal(
            barrier, inc=1, device_id=(peer // n_exp, peer % n_exp), device_id_type=MESH
        )
        return x

    lax.fori_loop(1, everyone, greet, 0)

    expert_row = lax.broadcasted_iota(jnp.int32, (LANES, tokens), 0)
    ids = ids_ref[...]
    mask_t = jnp.where((ids[0:1, :] == expert_row) | (ids[1:2, :] == expert_row), 1.0, 0.0)
    row = lax.broadcasted_iota(jnp.int32, (tokens, tokens), 0)
    col = lax.broadcasted_iota(jnp.int32, (tokens, tokens), 1)
    earlier = jnp.where(row < col, 1.0, 0.0).astype(jnp.bfloat16)
    before = jnp.dot(mask_t.astype(jnp.bfloat16), earlier, preferred_element_type=jnp.float32)
    slots[...] = jnp.where(mask_t > 0.5, before, -1.0)
    scale_in = 1.0 / jnp.max(hist_g_ref[...], axis=0, keepdims=True)
    scale_hidden = 1.0 / jnp.max(hist_h_ref[...], axis=0, keepdims=True)
    which = lax.broadcasted_iota(jnp.int32, (1, experts), 1)

    def pick(values, e):
        return jnp.sum(jnp.where(which == e, values, 0.0), axis=1, keepdims=True)

    position = lax.broadcasted_iota(jnp.int32, (capacity, tokens), 0).astype(jnp.float32)

    def prepare(e):
        onehot = jnp.where(slots[pl.ds(e, 1), :] == position, 1.0, 0.0).astype(jnp.bfloat16)
        rows = jnp.dot(onehot, grad_ref[...], preferred_element_type=jnp.float32)
        block = jnp.clip(rows * pick(scale_in, e), -1.0, 1.0)
        send[e] = block[0:main].astype(jnp.bfloat16)
        send_rest[e] = block[main:capacity].astype(jnp.bfloat16)

    def outgoing(d):
        return pltpu.make_async_remote_copy(
            src_ref=send.at[d // slices], dst_ref=recv.at[me],
            send_sem=send_sem.at[d], recv_sem=recv_sem.at[me],
            device_id=(my_dp, d), device_id_type=MESH,
        )

    def outgoing_rest(d):
        return pltpu.make_async_remote_copy(
            src_ref=send_rest.at[d // slices], dst_ref=recv_rest.at[me],
            send_sem=send_rest_sem.at[d], recv_sem=recv_rest_sem.at[me],
            device_id=(my_dp, d), device_id_type=MESH,
        )

    def incoming(s):
        return pltpu.make_async_remote_copy(
            src_ref=send.at[0], dst_ref=recv.at[s],
            send_sem=send_sem.at[s], recv_sem=recv_sem.at[s],
            device_id=(my_dp, s), device_id_type=MESH,
        )

    def incoming_rest(s):
        return pltpu.make_async_remote_copy(
            src_ref=send_rest.at[0], dst_ref=recv_rest.at[s],
            send_sem=send_rest_sem.at[s], recv_sem=recv_rest_sem.at[s],
            device_id=(my_dp, s), device_id_type=MESH,
        )

    def chip_of(j):
        k = jnp.where(j < 2, j, chips + 1 - j)
        if chips & (chips - 1) == 0:
            return flip_bits(q0, k, chips)
        return (q0 + k) % chips

    def source_of(j):
        if chips & (chips - 1) == 0:
            return chip_of(j)
        k = jnp.where(j < 2, j, chips + 1 - j)
        return (q0 + chips - k) % chips

    def prepare_pair(q):
        prepare(2 * q + c0)
        prepare(2 * q + 1 - c0)

    def send_pair(q):
        for c in (c0, 1 - c0):
            outgoing(2 * q + c).start()
            outgoing_rest(2 * q + c).start()

    greeted = everyone - 1
    if slices == 1:
        prepare_pair(chip_of(jnp.int32(1)))
        pl.semaphore_wait(barrier, greeted)

        def step(j, x):
            prepare_pair(chip_of((j + 1) % chips))
            send_pair(chip_of(j))
            return x
    else:
        def fill(e, x):
            prepare(e)
            return x

        lax.fori_loop(0, experts, fill, 0)
        pl.semaphore_wait(barrier, greeted)

        def step(j, x):
            send_pair(chip_of(j))
            return x

    lax.fori_loop(1, chips, step, 0)
    outgoing(partner).start()
    outgoing_rest(partner).start()

    recv[me] = send[own]
    recv_rest[me] = send_rest[own]
    row_peak = jnp.max(jnp.abs(grad_ref[...]).astype(jnp.float32), axis=1, keepdims=True)
    grad_peak = jnp.max(jnp.where(mask_t.T > 0.5, row_peak, 0.0), axis=0, keepdims=True)

    back = 1.0 / pick(scale_in, own)
    own_hidden = pick(scale_hidden, own)
    load.wait()

    def multiply(block):
        product = lax.dot_general(
            block, weight[...], (((1,), (1,)), ((), ())), preferred_element_type=jnp.float32
        )
        hidden = product * back
        scaled = jnp.clip(hidden * own_hidden, -1.0, 1.0)
        return scaled, jnp.max(jnp.max(jnp.abs(hidden), axis=0, keepdims=True), axis=1, keepdims=True)

    def pair_rows(q):
        return recv[pl.ds(2 * q, 2)].reshape(2 * main, recv.shape[2])

    def put_pair(q, scaled):
        for c in range(2):
            out_ref[2 * q + c, 0:main, :] = scaled[c * main:(c + 1) * main].astype(jnp.bfloat16)

    def take_own():
        incoming(partner).wait_recv()
        scaled, peak = multiply(pair_rows(q0))
        put_pair(q0, scaled)
        return peak

    def take(j, peak):
        q = source_of(j)
        incoming(2 * q).wait_recv()
        incoming(2 * q + 1).wait_recv()
        scaled, peak_here = multiply(pair_rows(q))
        put_pair(q, scaled)
        return jnp.maximum(peak, peak_here)

    peak = lax.fori_loop(1, chips - 1, take, take_own())

    def take_rest(j, x):
        incoming_rest((me + j) % n_exp).wait_recv()
        return x

    lax.fori_loop(1, n_exp, take_rest, 0)
    rest = capacity - main
    for s in range(n_exp):
        rest_rows[s * rest:(s + 1) * rest, :] = recv_rest[s].astype(jnp.float32)
    last = source_of(jnp.int32(chips - 1))
    incoming(2 * last).wait_recv()
    incoming(2 * last + 1).wait_recv()
    block = jnp.concatenate([pair_rows(last), rest_rows[...].astype(jnp.bfloat16)], axis=0)
    scaled, peak_here = multiply(block)
    peak = jnp.maximum(peak, peak_here)

    at = lax.broadcasted_iota(jnp.int32, (1, LANES), 1)
    hidden_peak = jnp.where(at == own, peak, 0.0)
    part = lax.broadcasted_iota(jnp.int32, (8, LANES), 0)
    mine[...] = jnp.where(part == 0, grad_peak, jnp.where(part == 1, hidden_peak, 0.0))

    def peak_copy(peer, slot, j):
        return pltpu.make_async_remote_copy(
            src_ref=mine, dst_ref=peaks_in.at[slot],
            send_sem=peak_send_sem.at[j], recv_sem=peak_recv_sem.at[slot],
            device_id=(peer // n_exp, peer % n_exp), device_id_type=MESH,
        )

    def peak_start(j, x):
        peak_copy((here + j) % everyone, here, j).start()
        return x

    def peak_fold(j, best):
        peer = (here + j) % everyone
        peak_copy(peer, peer, j).wait_recv()
        return jnp.maximum(best, peaks_in[peer])

    def peak_finish(j, x):
        peak_copy((here + j) % everyone, here, j).wait_send()
        return x

    lax.fori_loop(1, everyone, peak_start, 0)
    put_pair(last, scaled)
    for s in range(n_exp):
        at_row = 2 * main + s * rest
        out_ref[s, main:capacity, :] = scaled[at_row:at_row + rest].astype(jnp.bfloat16)
    best = lax.fori_loop(1, everyone, peak_fold, mine[...])
    lax.fori_loop(1, everyone, peak_finish, 0)

    keep = hist_g_ref.shape[0] - 1
    new_g_ref[0:keep, :] = hist_g_ref[1:keep + 1, :]
    new_g_ref[keep:keep + 1, :] = best[0:1, 0:experts]
    new_h_ref[0:keep, :] = hist_h_ref[1:keep + 1, :]
    new_h_ref[keep:keep + 1, :] = best[1:2, 0:experts]

    def drain(j, x):
        outgoing((me + j) % n_exp).wait_send()
        outgoing_rest((me + j) % n_exp).wait_send()
        return x

    lax.fori_loop(1, n_exp, drain, 0)


def per_device(grad_out, expert_ids, down_weight, history_grad, history_hidden):
    tokens, width = grad_out.shape
    experts = history_grad.shape[1]
    n_dp, n_exp = lax.axis_size("dp"), lax.axis_size("expert")
    capacity = tokens * 9 // 32
    main = (capacity - 1) // 16 * 16
    rest = capacity - main
    units = down_weight.shape[1]
    vmem = pl.BlockSpec(memory_space=pltpu.VMEM)
    dma = pltpu.SemaphoreType.DMA
    out, new_g, new_h = pl.pallas_call(
        functools.partial(kernel, n_dp, n_exp, experts, capacity),
        out_shape=(
            jax.ShapeDtypeStruct((n_exp, capacity, units), jnp.bfloat16),
            jax.ShapeDtypeStruct(history_grad.shape, jnp.float32),
            jax.ShapeDtypeStruct(history_hidden.shape, jnp.float32),
        ),
        in_specs=[vmem, vmem, vmem, vmem, pl.BlockSpec(memory_space=pl.ANY)],
        out_specs=(vmem, vmem, vmem),
        scratch_shapes=[
            pltpu.VMEM((units, width), jnp.bfloat16),
            pltpu.VMEM((experts, main, width), jnp.bfloat16),
            pltpu.VMEM((experts, rest, width), jnp.bfloat16),
            pltpu.VMEM((n_exp, main, width), jnp.bfloat16),
            pltpu.VMEM((n_exp, rest, width), jnp.bfloat16),
            pltpu.VMEM((n_exp * rest, width), jnp.float32),
            pltpu.VMEM((LANES, tokens), jnp.float32),
            pltpu.VMEM((8, LANES), jnp.float32),
            pltpu.VMEM((n_dp * n_exp, 8, LANES), jnp.float32),
            dma, dma((n_exp,)), dma((n_exp,)), dma((n_exp,)), dma((n_exp,)),
            dma((n_dp * n_exp,)), dma((n_dp * n_exp,)),
        ],
        compiler_params=pltpu.CompilerParams(
            collective_id=0, has_side_effects=True, vmem_limit_bytes=60 * 1024 * 1024
        ),
    )(grad_out, expert_ids.T, history_grad, history_hidden, down_weight)
    return out.reshape(1, 1, n_exp * capacity, units), new_g, new_h


def solution(mesh):
    in_specs = (
        P(("dp", "expert"), None),
        P(("dp", "expert"), None),
        P("expert", None, None),
        P(),
        P(),
    )
    out_specs = (P("dp", "expert", None, None), P(), P())
    return jax.shard_map(
        per_device, mesh=mesh, in_specs=in_specs, out_specs=out_specs, check_vma=False
    )
```

```python
import functools

import jax
import jax.numpy as jnp
from jax import lax
from jax.experimental import pallas as pl
from jax.experimental.pallas import tpu as pltpu
from jax.sharding import PartitionSpec as P

MESH = pl.DeviceIdType.MESH
LANES = 128


def flip_bits(q, k, count):
    out, bit = 0, 1
    while bit < count:
        a, b = (q // bit) % 2, (k // bit) % 2
        out = out + bit * (a + b - 2 * a * b)
        bit *= 2
    return out


def kernel(
    n_dp, n_exp, experts, capacity,
    grad_ref, ids_ref, hist_g_ref, hist_h_ref, weight_hbm,
    out_ref, best_ref,
    held, weight, send, send_rest, recv, recv_rest, rest_rows, slots, mine, peaks_in,
    weight_sem, send_sem, recv_sem, send_rest_sem, recv_rest_sem, peak_send_sem, peak_recv_sem,
):
    tokens = grad_ref.shape[0]
    main = send.shape[1]
    slices = n_exp // experts
    chips = n_exp // 2
    my_dp, me = lax.axis_index("dp"), lax.axis_index("expert")
    q0, c0 = me // 2, me % 2
    partner = q0 * 2 + 1 - c0
    own = me // slices
    load = pltpu.make_async_copy(weight_hbm.at[0], weight, weight_sem)
    load.start()

    barrier = pltpu.get_barrier_semaphore()

    everyone = n_dp * n_exp
    here = my_dp * n_exp + me

    def greet(j, x):
        peer = (here + j) % everyone
        pl.semaphore_signal(
            barrier, inc=1, device_id=(peer // n_exp, peer % n_exp), device_id_type=MESH
        )
        return x

    lax.fori_loop(1, everyone, greet, 0)

    expert_row = lax.broadcasted_iota(jnp.int32, (LANES, tokens), 0)
    ids = ids_ref[...]
    mask_t = jnp.where((ids[0:1, :] == expert_row) | (ids[1:2, :] == expert_row), 1.0, 0.0)
    row = lax.broadcasted_iota(jnp.int32, (tokens, tokens), 0)
    col = lax.broadcasted_iota(jnp.int32, (tokens, tokens), 1)
    earlier = jnp.where(row < col, 1.0, 0.0).astype(jnp.bfloat16)
    before = jnp.dot(mask_t.astype(jnp.bfloat16), earlier, preferred_element_type=jnp.float32)
    slots[...] = jnp.where(mask_t > 0.5, before, -1.0)
    scale_in = 1.0 / jnp.max(hist_g_ref[...], axis=0, keepdims=True)
    scale_hidden = 1.0 / jnp.max(hist_h_ref[...], axis=0, keepdims=True)
    which = lax.broadcasted_iota(jnp.int32, (1, experts), 1)

    def pick(values, e):
        return jnp.sum(jnp.where(which == e, values, 0.0), axis=1, keepdims=True)

    position = lax.broadcasted_iota(jnp.int32, (capacity, tokens), 0).astype(jnp.float32)

    def prepare(e):
        onehot = jnp.where(slots[pl.ds(e, 1), :] == position, 1.0, 0.0).astype(jnp.bfloat16)
        rows = jnp.dot(onehot, grad_ref[...], preferred_element_type=jnp.float32)
        block = jnp.clip(rows * pick(scale_in, e), -1.0, 1.0)
        send[e] = block[0:main].astype(jnp.bfloat16)
        send_rest[e] = block[main:capacity].astype(jnp.bfloat16)

    def outgoing(d):
        return pltpu.make_async_remote_copy(
            src_ref=send.at[d // slices], dst_ref=recv.at[me],
            send_sem=send_sem.at[d], recv_sem=recv_sem.at[me],
            device_id=(my_dp, d), device_id_type=MESH,
        )

    def outgoing_rest(d):
        return pltpu.make_async_remote_copy(
            src_ref=send_rest.at[d // slices], dst_ref=recv_rest.at[me],
            send_sem=send_rest_sem.at[d], recv_sem=recv_rest_sem.at[me],
            device_id=(my_dp, d), device_id_type=MESH,
        )

    def incoming(s):
        return pltpu.make_async_remote_copy(
            src_ref=send.at[0], dst_ref=recv.at[s],
            send_sem=send_sem.at[s], recv_sem=recv_sem.at[s],
            device_id=(my_dp, s), device_id_type=MESH,
        )

    def incoming_rest(s):
        return pltpu.make_async_remote_copy(
            src_ref=send_rest.at[0], dst_ref=recv_rest.at[s],
            send_sem=send_rest_sem.at[s], recv_sem=recv_rest_sem.at[s],
            device_id=(my_dp, s), device_id_type=MESH,
        )

    def chip_of(j):
        k = j
        if chips & (chips - 1) == 0:
            return flip_bits(q0, k, chips)
        return (q0 + k) % chips

    def source_of(j):
        if chips & (chips - 1) == 0:
            return chip_of(j)
        k = j
        return (q0 + chips - k) % chips

    def prepare_pair(q):
        prepare(2 * q + c0)
        prepare(2 * q + 1 - c0)

    def send_pair(q):
        for c in (c0, 1 - c0):
            outgoing(2 * q + c).start()
            outgoing_rest(2 * q + c).start()

    greeted = everyone - 1
    if slices == 1:
        prepare_pair(chip_of(jnp.int32(1)))
        pl.semaphore_wait(barrier, greeted)

        def step(j, x):
            prepare_pair(chip_of((j + 1) % chips))
            send_pair(chip_of(j))
            return x
    else:
        def fill(e, x):
            prepare(e)
            return x

        lax.fori_loop(0, experts, fill, 0)
        pl.semaphore_wait(barrier, greeted)

        def step(j, x):
            send_pair(chip_of(j))
            return x

    lax.fori_loop(1, chips, step, 0)
    outgoing(partner).start()
    outgoing_rest(partner).start()

    recv[me] = send[own]
    recv_rest[me] = send_rest[own]
    row_peak = jnp.max(jnp.abs(grad_ref[...]).astype(jnp.float32), axis=1, keepdims=True)
    grad_peak = jnp.max(jnp.where(mask_t.T > 0.5, row_peak, 0.0), axis=0, keepdims=True)

    back = 1.0 / pick(scale_in, own)
    own_hidden = pick(scale_hidden, own)
    load.wait()

    def multiply(block):
        product = lax.dot_general(
            block, weight[...], (((1,), (1,)), ((), ())), preferred_element_type=jnp.float32
        )
        hidden = product * back
        scaled = jnp.clip(hidden * own_hidden, -1.0, 1.0)
        return scaled, jnp.max(jnp.max(jnp.abs(hidden), axis=0, keepdims=True), axis=1, keepdims=True)

    def pair_rows(q):
        return recv[pl.ds(2 * q, 2)].reshape(2 * main, recv.shape[2])

    def put_pair(q, scaled):
        for c in range(2):
            held[2 * q + c] = scaled[c * main:(c + 1) * main].astype(jnp.bfloat16)

    def take_own():
        incoming(partner).wait_recv()
        scaled, peak = multiply(pair_rows(q0))
        put_pair(q0, scaled)
        return peak

    def take(j, peak):
        q = source_of(j)
        incoming(2 * q).wait_recv()
        incoming(2 * q + 1).wait_recv()
        scaled, peak_here = multiply(pair_rows(q))
        put_pair(q, scaled)
        return jnp.maximum(peak, peak_here)

    peak = lax.fori_loop(1, chips - 1, take, take_own())

    def take_rest(j, x):
        incoming_rest((me + j) % n_exp).wait_recv()
        return x

    lax.fori_loop(1, n_exp, take_rest, 0)
    rest = capacity - main
    for s in range(n_exp):
        rest_rows[s * rest:(s + 1) * rest, :] = recv_rest[s].astype(jnp.float32)
    last = source_of(jnp.int32(chips - 1))
    incoming(2 * last).wait_recv()
    incoming(2 * last + 1).wait_recv()
    block = jnp.concatenate([pair_rows(last), rest_rows[...].astype(jnp.bfloat16)], axis=0)
    scaled, peak_here = multiply(block)
    peak = jnp.maximum(peak, peak_here)

    at = lax.broadcasted_iota(jnp.int32, (1, LANES), 1)
    hidden_peak = jnp.where(at == own, peak, 0.0)
    part = lax.broadcasted_iota(jnp.int32, (8, LANES), 0)
    mine[...] = jnp.where(part == 0, grad_peak, jnp.where(part == 1, hidden_peak, 0.0))

    def peak_copy(peer, slot, j):
        return pltpu.make_async_remote_copy(
            src_ref=mine, dst_ref=peaks_in.at[slot],
            send_sem=peak_send_sem.at[j], recv_sem=peak_recv_sem.at[slot],
            device_id=(peer // n_exp, peer % n_exp), device_id_type=MESH,
        )

    def peak_start(j, x):
        peak_copy((here + j) % everyone, here, j).start()
        return x

    def peak_fold(j, best):
        peer = (here + j) % everyone
        peak_copy(peer, peer, j).wait_recv()
        return jnp.maximum(best, peaks_in[peer])

    def peak_finish(j, x):
        peak_copy((here + j) % everyone, here, j).wait_send()
        return x

    lax.fori_loop(1, everyone, peak_start, 0)
    put_pair(last, scaled)
    for s in range(n_exp):
        at_row = 2 * main + s * rest
        base = s * capacity
        out_ref[base:base + main, :] = held[s]
        out_ref[base + main:base + capacity, :] = scaled[at_row:at_row + rest].astype(jnp.bfloat16)
    best = lax.fori_loop(1, everyone, peak_fold, mine[...])
    lax.fori_loop(1, everyone, peak_finish, 0)

    best_ref[...] = best

    def drain(j, x):
        outgoing((me + j) % n_exp).wait_send()
        outgoing_rest((me + j) % n_exp).wait_send()
        return x

    lax.fori_loop(1, n_exp, drain, 0)


def finish_kernel(hist_g_ref, hist_h_ref, best_ref, out_ref, new_g_ref, new_h_ref, final_ref):
    final_ref[...] = out_ref[...]
    keep = hist_g_ref.shape[0] - 1
    experts = hist_g_ref.shape[1]
    new_g_ref[0:keep, :] = hist_g_ref[1:keep + 1, :]
    new_g_ref[keep:keep + 1, :] = best_ref[0:1, 0:experts]
    new_h_ref[0:keep, :] = hist_h_ref[1:keep + 1, :]
    new_h_ref[keep:keep + 1, :] = best_ref[1:2, 0:experts]


def per_device(grad_out, expert_ids, down_weight, history_grad, history_hidden):
    tokens, width = grad_out.shape
    experts = history_grad.shape[1]
    n_dp, n_exp = lax.axis_size("dp"), lax.axis_size("expert")
    capacity = tokens * 9 // 32
    main = (capacity - 1) // 16 * 16
    rest = capacity - main
    units = down_weight.shape[1]
    vmem = pl.BlockSpec(memory_space=pltpu.VMEM)
    dma = pltpu.SemaphoreType.DMA
    out, best = pl.pallas_call(
        functools.partial(kernel, n_dp, n_exp, experts, capacity),
        out_shape=(
            jax.ShapeDtypeStruct((n_exp * capacity, units), jnp.bfloat16),
            jax.ShapeDtypeStruct((8, LANES), jnp.float32),
        ),
        in_specs=[vmem, vmem, vmem, vmem, pl.BlockSpec(memory_space=pl.ANY)],
        out_specs=(vmem, vmem),
        scratch_shapes=[
            pltpu.VMEM((n_exp, main, units), jnp.bfloat16),
            pltpu.VMEM((units, width), jnp.bfloat16),
            pltpu.VMEM((experts, main, width), jnp.bfloat16),
            pltpu.VMEM((experts, rest, width), jnp.bfloat16),
            pltpu.VMEM((n_exp, main, width), jnp.bfloat16),
            pltpu.VMEM((n_exp, rest, width), jnp.bfloat16),
            pltpu.VMEM((n_exp * rest, width), jnp.float32),
            pltpu.VMEM((LANES, tokens), jnp.float32),
            pltpu.VMEM((8, LANES), jnp.float32),
            pltpu.VMEM((n_dp * n_exp, 8, LANES), jnp.float32),
            dma, dma((n_exp,)), dma((n_exp,)), dma((n_exp,)), dma((n_exp,)),
            dma((n_dp * n_exp,)), dma((n_dp * n_exp,)),
        ],
        compiler_params=pltpu.CompilerParams(
            collective_id=0, has_side_effects=True, vmem_limit_bytes=60 * 1024 * 1024
        ),
    )(grad_out, expert_ids.T, history_grad, history_hidden, down_weight)
    new_g, new_h, out = pl.pallas_call(
        finish_kernel,
        out_shape=(
            jax.ShapeDtypeStruct(history_grad.shape, jnp.float32),
            jax.ShapeDtypeStruct(history_hidden.shape, jnp.float32),
            jax.ShapeDtypeStruct(out.shape, out.dtype),
        ),
        in_specs=[vmem, vmem, vmem, vmem],
        out_specs=(vmem, vmem, vmem),
    )(history_grad, history_hidden, best, out)
    return out.reshape(1, 1, n_exp * capacity, units), new_g, new_h


def solution(mesh):
    in_specs = (
        P(("dp", "expert"), None),
        P(("dp", "expert"), None),
        P("expert", None, None),
        P(),
        P(),
    )
    out_specs = (P("dp", "expert", None, None), P(), P())
    return jax.shard_map(
        per_device, mesh=mesh, in_specs=in_specs, out_specs=out_specs, check_vma=False
    )
```

```python
import functools

import jax
import jax.numpy as jnp
from jax import lax
from jax.experimental import pallas as pl
from jax.experimental.pallas import tpu as pltpu
from jax.sharding import PartitionSpec as P

MESH = pl.DeviceIdType.MESH
PARTS = 4
LANES = 128


def flip_bits(q, k, count):
    out, bit = 0, 1
    while bit < count:
        a, b = (q // bit) % 2, (k // bit) % 2
        out = out + bit * (a + b - 2 * a * b)
        bit *= 2
    return out


def kernel(
    n_dp, n_exp, experts, capacity,
    grad_ref, ids_ref, hist_g_ref, hist_h_ref, weight_hbm,
    out_ref, best_ref,
    held, weight, send, send_rest, recv, recv_rest, rest_rows, slots, mine, peaks_in,
    weight_sem, send_sem, recv_sem, send_rest_sem, recv_rest_sem, peak_send_sem, peak_recv_sem,
):
    tokens = grad_ref.shape[0]
    main = send.shape[1]
    slices = n_exp // experts
    chips = n_exp // 2
    my_dp, me = lax.axis_index("dp"), lax.axis_index("expert")
    q0, c0 = me // 2, me % 2
    partner = q0 * 2 + 1 - c0
    own = me // slices
    load = pltpu.make_async_copy(weight_hbm.at[0], weight, weight_sem)
    load.start()

    barrier = pltpu.get_barrier_semaphore()

    everyone = n_dp * n_exp
    here = my_dp * n_exp + me

    def greet(j, x):
        peer = (here + j) % everyone
        pl.semaphore_signal(
            barrier, inc=1, device_id=(peer // n_exp, peer % n_exp), device_id_type=MESH
        )
        return x

    lax.fori_loop(1, everyone, greet, 0)

    expert_row = lax.broadcasted_iota(jnp.int32, (LANES, tokens), 0)
    ids = ids_ref[...]
    mask_t = jnp.where((ids[0:1, :] == expert_row) | (ids[1:2, :] == expert_row), 1.0, 0.0)
    row = lax.broadcasted_iota(jnp.int32, (tokens, tokens), 0)
    col = lax.broadcasted_iota(jnp.int32, (tokens, tokens), 1)
    earlier = jnp.where(row < col, 1.0, 0.0).astype(jnp.bfloat16)
    before = jnp.dot(mask_t.astype(jnp.bfloat16), earlier, preferred_element_type=jnp.float32)
    slots[...] = jnp.where(mask_t > 0.5, before, -1.0)
    scale_in = 1.0 / jnp.max(hist_g_ref[...], axis=0, keepdims=True)
    scale_hidden = 1.0 / jnp.max(hist_h_ref[...], axis=0, keepdims=True)
    which = lax.broadcasted_iota(jnp.int32, (1, experts), 1)

    def pick(values, e):
        return jnp.sum(jnp.where(which == e, values, 0.0), axis=1, keepdims=True)

    position = lax.broadcasted_iota(jnp.int32, (capacity, tokens), 0).astype(jnp.float32)

    def prepare(e):
        onehot = jnp.where(slots[pl.ds(e, 1), :] == position, 1.0, 0.0).astype(jnp.bfloat16)
        rows = jnp.dot(onehot, grad_ref[...], preferred_element_type=jnp.float32)
        block = jnp.clip(rows * pick(scale_in, e), -1.0, 1.0)
        send[e] = block[0:main].astype(jnp.bfloat16)
        send_rest[e] = block[main:capacity].astype(jnp.bfloat16)

    span = weight.shape[1] // PARTS

    def outgoing(d, p):
        columns = pl.ds(p * span, span)
        return pltpu.make_async_remote_copy(
            src_ref=send.at[d // slices, :, columns], dst_ref=recv.at[me, :, columns],
            send_sem=send_sem.at[p, d], recv_sem=recv_sem.at[p, me],
            device_id=(my_dp, d), device_id_type=MESH,
        )

    def outgoing_rest(d):
        return pltpu.make_async_remote_copy(
            src_ref=send_rest.at[d // slices], dst_ref=recv_rest.at[me],
            send_sem=send_rest_sem.at[d], recv_sem=recv_rest_sem.at[me],
            device_id=(my_dp, d), device_id_type=MESH,
        )

    def incoming(s, p):
        columns = pl.ds(p * span, span)
        return pltpu.make_async_remote_copy(
            src_ref=send.at[0, :, columns], dst_ref=recv.at[s, :, columns],
            send_sem=send_sem.at[p, s], recv_sem=recv_sem.at[p, s],
            device_id=(my_dp, s), device_id_type=MESH,
        )

    def incoming_rest(s):
        return pltpu.make_async_remote_copy(
            src_ref=send_rest.at[0], dst_ref=recv_rest.at[s],
            send_sem=send_rest_sem.at[s], recv_sem=recv_rest_sem.at[s],
            device_id=(my_dp, s), device_id_type=MESH,
        )

    def chip_of(j):
        k = j
        if chips & (chips - 1) == 0:
            return flip_bits(q0, k, chips)
        return (q0 + k) % chips

    def source_of(j):
        if chips & (chips - 1) == 0:
            return chip_of(j)
        k = j
        return (q0 + chips - k) % chips

    def prepare_pair(q):
        prepare(2 * q + c0)
        prepare(2 * q + 1 - c0)

    def send_pair(q):
        for p in range(PARTS):
            for c in (c0, 1 - c0):
                outgoing(2 * q + c, p).start()
                if p == 0:
                    outgoing_rest(2 * q + c).start()

    greeted = everyone - 1
    if slices == 1:
        prepare_pair(chip_of(jnp.int32(1)))
        pl.semaphore_wait(barrier, greeted)

        def step(j, x):
            prepare_pair(chip_of((j + 1) % chips))
            send_pair(chip_of(j))
            return x
    else:
        def fill(e, x):
            prepare(e)
            return x

        lax.fori_loop(0, experts, fill, 0)
        pl.semaphore_wait(barrier, greeted)

        def step(j, x):
            send_pair(chip_of(j))
            return x

    lax.fori_loop(1, chips, step, 0)
    for p in range(PARTS):
        outgoing(partner, p).start()
    outgoing_rest(partner).start()

    recv[me] = send[own]
    recv_rest[me] = send_rest[own]
    row_peak = jnp.max(jnp.abs(grad_ref[...]).astype(jnp.float32), axis=1, keepdims=True)
    grad_peak = jnp.max(jnp.where(mask_t.T > 0.5, row_peak, 0.0), axis=0, keepdims=True)

    back = 1.0 / pick(scale_in, own)
    own_hidden = pick(scale_hidden, own)
    load.wait()

    def times_weight(block, columns):
        return lax.dot_general(
            block, weight[:, columns], (((1,), (1,)), ((), ())), preferred_element_type=jnp.float32
        )

    def multiply(block):
        return finish(times_weight(block, slice(None)))

    def finish(product):
        hidden = product * back
        scaled = jnp.clip(hidden * own_hidden, -1.0, 1.0)
        return scaled, jnp.max(jnp.max(jnp.abs(hidden), axis=0, keepdims=True), axis=1, keepdims=True)

    def pair_rows(q):
        return recv[pl.ds(2 * q, 2)].reshape(2 * main, recv.shape[2])

    def put_pair(q, scaled):
        for c in range(2):
            held[2 * q + c] = scaled[c * main:(c + 1) * main].astype(jnp.bfloat16)

    def take_own():
        for p in range(PARTS):
            incoming(partner, p).wait_recv()
        scaled, peak = multiply(pair_rows(q0))
        put_pair(q0, scaled)
        return peak

    def take(j, peak):
        q = source_of(j)
        for p in range(PARTS):
            incoming(2 * q, p).wait_recv()
            incoming(2 * q + 1, p).wait_recv()
        scaled, peak_here = multiply(pair_rows(q))
        put_pair(q, scaled)
        return jnp.maximum(peak, peak_here)

    peak = lax.fori_loop(1, chips - 1, take, take_own())

    def take_rest(j, x):
        incoming_rest((me + j) % n_exp).wait_recv()
        return x

    lax.fori_loop(1, n_exp, take_rest, 0)
    rest = capacity - main
    for s in range(n_exp):
        rest_rows[s * rest:(s + 1) * rest, :] = recv_rest[s].astype(jnp.float32)
    last = source_of(jnp.int32(chips - 1))
    product = None
    for p in range(PARTS):
        incoming(2 * last, p).wait_recv()
        incoming(2 * last + 1, p).wait_recv()
        columns = slice(p * span, (p + 1) * span)
        pair = recv[pl.ds(2 * last, 2), :, columns].reshape(2 * main, span)
        block = jnp.concatenate([pair, rest_rows[:, columns].astype(jnp.bfloat16)], axis=0)
        piece = times_weight(block, columns)
        product = piece if product is None else product + piece
    scaled, peak_here = finish(product)
    peak = jnp.maximum(peak, peak_here)

    at = lax.broadcasted_iota(jnp.int32, (1, LANES), 1)
    hidden_peak = jnp.where(at == own, peak, 0.0)
    part = lax.broadcasted_iota(jnp.int32, (8, LANES), 0)
    mine[...] = jnp.where(part == 0, grad_peak, jnp.where(part == 1, hidden_peak, 0.0))

    def peak_copy(peer, slot, j):
        return pltpu.make_async_remote_copy(
            src_ref=mine, dst_ref=peaks_in.at[slot],
            send_sem=peak_send_sem.at[j], recv_sem=peak_recv_sem.at[slot],
            device_id=(peer // n_exp, peer % n_exp), device_id_type=MESH,
        )

    def peak_start(j, x):
        peak_copy((here + j) % everyone, here, j).start()
        return x

    def peak_fold(j, best):
        peer = (here + j) % everyone
        peak_copy(peer, peer, j).wait_recv()
        return jnp.maximum(best, peaks_in[peer])

    def peak_finish(j, x):
        peak_copy((here + j) % everyone, here, j).wait_send()
        return x

    lax.fori_loop(1, everyone, peak_start, 0)
    put_pair(last, scaled)
    for s in range(n_exp):
        at_row = 2 * main + s * rest
        base = s * capacity
        out_ref[base:base + main, :] = held[s]
        out_ref[base + main:base + capacity, :] = scaled[at_row:at_row + rest].astype(jnp.bfloat16)
    best = lax.fori_loop(1, everyone, peak_fold, mine[...])
    lax.fori_loop(1, everyone, peak_finish, 0)

    best_ref[...] = best

    def drain(j, x):
        for p in range(PARTS):
            outgoing((me + j) % n_exp, p).wait_send()
        outgoing_rest((me + j) % n_exp).wait_send()
        return x

    lax.fori_loop(1, n_exp, drain, 0)


def finish_kernel(hist_g_ref, hist_h_ref, best_ref, out_ref, new_g_ref, new_h_ref, final_ref):
    final_ref[...] = out_ref[...]
    keep = hist_g_ref.shape[0] - 1
    experts = hist_g_ref.shape[1]
    new_g_ref[0:keep, :] = hist_g_ref[1:keep + 1, :]
    new_g_ref[keep:keep + 1, :] = best_ref[0:1, 0:experts]
    new_h_ref[0:keep, :] = hist_h_ref[1:keep + 1, :]
    new_h_ref[keep:keep + 1, :] = best_ref[1:2, 0:experts]


def per_device(grad_out, expert_ids, down_weight, history_grad, history_hidden):
    tokens, width = grad_out.shape
    experts = history_grad.shape[1]
    n_dp, n_exp = lax.axis_size("dp"), lax.axis_size("expert")
    capacity = tokens * 9 // 32
    main = (capacity - 1) // 16 * 16
    rest = capacity - main
    units = down_weight.shape[1]
    vmem = pl.BlockSpec(memory_space=pltpu.VMEM)
    dma = pltpu.SemaphoreType.DMA
    out, best = pl.pallas_call(
        functools.partial(kernel, n_dp, n_exp, experts, capacity),
        out_shape=(
            jax.ShapeDtypeStruct((n_exp * capacity, units), jnp.bfloat16),
            jax.ShapeDtypeStruct((8, LANES), jnp.float32),
        ),
        in_specs=[vmem, vmem, vmem, vmem, pl.BlockSpec(memory_space=pl.ANY)],
        out_specs=(vmem, vmem),
        scratch_shapes=[
            pltpu.VMEM((n_exp, main, units), jnp.bfloat16),
            pltpu.VMEM((units, width), jnp.bfloat16),
            pltpu.VMEM((experts, main, width), jnp.bfloat16),
            pltpu.VMEM((experts, rest, width), jnp.bfloat16),
            pltpu.VMEM((n_exp, main, width), jnp.bfloat16),
            pltpu.VMEM((n_exp, rest, width), jnp.bfloat16),
            pltpu.VMEM((n_exp * rest, width), jnp.float32),
            pltpu.VMEM((LANES, tokens), jnp.float32),
            pltpu.VMEM((8, LANES), jnp.float32),
            pltpu.VMEM((n_dp * n_exp, 8, LANES), jnp.float32),
            dma, dma((PARTS, n_exp)), dma((PARTS, n_exp)), dma((n_exp,)), dma((n_exp,)),
            dma((n_dp * n_exp,)), dma((n_dp * n_exp,)),
        ],
        compiler_params=pltpu.CompilerParams(
            collective_id=0, has_side_effects=True, vmem_limit_bytes=60 * 1024 * 1024
        ),
    )(grad_out, expert_ids.T, history_grad, history_hidden, down_weight)
    new_g, new_h, out = pl.pallas_call(
        finish_kernel,
        out_shape=(
            jax.ShapeDtypeStruct(history_grad.shape, jnp.float32),
            jax.ShapeDtypeStruct(history_hidden.shape, jnp.float32),
            jax.ShapeDtypeStruct(out.shape, out.dtype),
        ),
        in_specs=[vmem, vmem, vmem, vmem],
        out_specs=(vmem, vmem, vmem),
    )(history_grad, history_hidden, best, out)
    return out.reshape(1, 1, n_exp * capacity, units), new_g, new_h


def solution(mesh):
    in_specs = (
        P(("dp", "expert"), None),
        P(("dp", "expert"), None),
        P("expert", None, None),
        P(),
        P(),
    )
    out_specs = (P("dp", "expert", None, None), P(), P())
    return jax.shard_map(
        per_device, mesh=mesh, in_specs=in_specs, out_specs=out_specs, check_vma=False
    )
```

```python
import functools

import jax
import jax.numpy as jnp
from jax import lax
from jax.experimental import pallas as pl
from jax.experimental.pallas import tpu as pltpu
from jax.sharding import PartitionSpec as P

MESH = pl.DeviceIdType.MESH
PARTS = 4
LANES = 128


def flip_bits(q, k, count):
    out, bit = 0, 1
    while bit < count:
        a, b = (q // bit) % 2, (k // bit) % 2
        out = out + bit * (a + b - 2 * a * b)
        bit *= 2
    return out


def kernel(
    n_dp, n_exp, experts, capacity,
    grad_hbm, ids_ref, hist_g_ref, hist_h_ref, weight_hbm,
    out_ref, best_ref,
    grad_ref, held, weight, send, send_rest, recv, recv_rest, rest_rows, slots, mine, peaks_in,
    grad_sem, weight_sem, send_sem, recv_sem, send_rest_sem, recv_rest_sem, peak_send_sem, peak_recv_sem,
):
    tokens = grad_ref.shape[0]
    main = send.shape[1]
    slices = n_exp // experts
    chips = n_exp // 2
    my_dp, me = lax.axis_index("dp"), lax.axis_index("expert")
    q0, c0 = me // 2, me % 2
    partner = q0 * 2 + 1 - c0
    own = me // slices
    grad_load = pltpu.make_async_copy(grad_hbm, grad_ref, grad_sem)
    grad_load.start()
    load = pltpu.make_async_copy(weight_hbm.at[0], weight, weight_sem)

    barrier = pltpu.get_barrier_semaphore()

    everyone = n_dp * n_exp
    here = my_dp * n_exp + me

    def greet(j, x):
        peer = (here + j) % everyone
        pl.semaphore_signal(
            barrier, inc=1, device_id=(peer // n_exp, peer % n_exp), device_id_type=MESH
        )
        return x

    lax.fori_loop(1, everyone, greet, 0)

    expert_row = lax.broadcasted_iota(jnp.int32, (LANES, tokens), 0)
    ids = ids_ref[...]
    mask_t = jnp.where((ids[0:1, :] == expert_row) | (ids[1:2, :] == expert_row), 1.0, 0.0)
    row = lax.broadcasted_iota(jnp.int32, (tokens, tokens), 0)
    col = lax.broadcasted_iota(jnp.int32, (tokens, tokens), 1)
    earlier = jnp.where(row < col, 1.0, 0.0).astype(jnp.bfloat16)
    before = jnp.dot(mask_t.astype(jnp.bfloat16), earlier, preferred_element_type=jnp.float32)
    slots[...] = jnp.where(mask_t > 0.5, before, -1.0)
    scale_in = 1.0 / jnp.max(hist_g_ref[...], axis=0, keepdims=True)
    scale_hidden = 1.0 / jnp.max(hist_h_ref[...], axis=0, keepdims=True)
    which = lax.broadcasted_iota(jnp.int32, (1, experts), 1)

    def pick(values, e):
        return jnp.sum(jnp.where(which == e, values, 0.0), axis=1, keepdims=True)

    position = lax.broadcasted_iota(jnp.int32, (capacity, tokens), 0).astype(jnp.float32)

    def prepare(e):
        onehot = jnp.where(slots[pl.ds(e, 1), :] == position, 1.0, 0.0).astype(jnp.bfloat16)
        rows = jnp.dot(onehot, grad_ref[...], preferred_element_type=jnp.float32)
        block = jnp.clip(rows * pick(scale_in, e), -1.0, 1.0)
        send[e] = block[0:main].astype(jnp.bfloat16)
        send_rest[e] = block[main:capacity].astype(jnp.bfloat16)

    span = weight.shape[1] // PARTS

    def outgoing(d, p):
        columns = pl.ds(p * span, span)
        return pltpu.make_async_remote_copy(
            src_ref=send.at[d // slices, :, columns], dst_ref=recv.at[me, :, columns],
            send_sem=send_sem.at[p, d], recv_sem=recv_sem.at[p, me],
            device_id=(my_dp, d), device_id_type=MESH,
        )

    def outgoing_rest(d):
        return pltpu.make_async_remote_copy(
            src_ref=send_rest.at[d // slices], dst_ref=recv_rest.at[me],
            send_sem=send_rest_sem.at[d], recv_sem=recv_rest_sem.at[me],
            device_id=(my_dp, d), device_id_type=MESH,
        )

    def incoming(s, p):
        columns = pl.ds(p * span, span)
        return pltpu.make_async_remote_copy(
            src_ref=send.at[0, :, columns], dst_ref=recv.at[s, :, columns],
            send_sem=send_sem.at[p, s], recv_sem=recv_sem.at[p, s],
            device_id=(my_dp, s), device_id_type=MESH,
        )

    def incoming_rest(s):
        return pltpu.make_async_remote_copy(
            src_ref=send_rest.at[0], dst_ref=recv_rest.at[s],
            send_sem=send_rest_sem.at[s], recv_sem=recv_rest_sem.at[s],
            device_id=(my_dp, s), device_id_type=MESH,
        )

    def chip_of(j):
        k = j
        if chips & (chips - 1) == 0:
            return flip_bits(q0, k, chips)
        return (q0 + k) % chips

    def source_of(j):
        if chips & (chips - 1) == 0:
            return chip_of(j)
        k = j
        return (q0 + chips - k) % chips

    def prepare_pair(q):
        prepare(2 * q + c0)
        prepare(2 * q + 1 - c0)

    def send_pair(q):
        for p in range(PARTS):
            for c in (c0, 1 - c0):
                outgoing(2 * q + c, p).start()
                if p == 0:
                    outgoing_rest(2 * q + c).start()

    greeted = everyone - 1
    grad_load.wait()
    load.start()
    if slices == 1:
        prepare_pair(chip_of(jnp.int32(1)))
        pl.semaphore_wait(barrier, greeted)

        def step(j, x):
            prepare_pair(chip_of((j + 1) % chips))
            send_pair(chip_of(j))
            return x
    else:
        def fill(e, x):
            prepare(e)
            return x

        lax.fori_loop(0, experts, fill, 0)
        pl.semaphore_wait(barrier, greeted)

        def step(j, x):
            send_pair(chip_of(j))
            return x

    lax.fori_loop(1, chips, step, 0)
    for p in range(PARTS):
        outgoing(partner, p).start()
    outgoing_rest(partner).start()

    recv[me] = send[own]
    recv_rest[me] = send_rest[own]
    row_peak = jnp.max(jnp.abs(grad_ref[...]).astype(jnp.float32), axis=1, keepdims=True)
    grad_peak = jnp.max(jnp.where(mask_t.T > 0.5, row_peak, 0.0), axis=0, keepdims=True)

    back = 1.0 / pick(scale_in, own)
    own_hidden = pick(scale_hidden, own)
    load.wait()

    def times_weight(block, columns):
        return lax.dot_general(
            block, weight[:, columns], (((1,), (1,)), ((), ())), preferred_element_type=jnp.float32
        )

    def multiply(block):
        return finish(times_weight(block, slice(None)))

    def finish(product):
        hidden = product * back
        scaled = jnp.clip(hidden * own_hidden, -1.0, 1.0)
        return scaled, jnp.max(jnp.max(jnp.abs(hidden), axis=0, keepdims=True), axis=1, keepdims=True)

    def pair_rows(q):
        return recv[pl.ds(2 * q, 2)].reshape(2 * main, recv.shape[2])

    def put_pair(q, scaled):
        for c in range(2):
            held[2 * q + c] = scaled[c * main:(c + 1) * main].astype(jnp.bfloat16)

    def take_own():
        for p in range(PARTS):
            incoming(partner, p).wait_recv()
        scaled, peak = multiply(pair_rows(q0))
        put_pair(q0, scaled)
        return peak

    def take(j, peak):
        q = source_of(j)
        for p in range(PARTS):
            incoming(2 * q, p).wait_recv()
            incoming(2 * q + 1, p).wait_recv()
        scaled, peak_here = multiply(pair_rows(q))
        put_pair(q, scaled)
        return jnp.maximum(peak, peak_here)

    peak = lax.fori_loop(1, chips - 1, take, take_own())

    def take_rest(j, x):
        incoming_rest((me + j) % n_exp).wait_recv()
        return x

    lax.fori_loop(1, n_exp, take_rest, 0)
    rest = capacity - main
    for s in range(n_exp):
        rest_rows[s * rest:(s + 1) * rest, :] = recv_rest[s].astype(jnp.float32)
    last = source_of(jnp.int32(chips - 1))
    product = None
    for p in range(PARTS):
        incoming(2 * last, p).wait_recv()
        incoming(2 * last + 1, p).wait_recv()
        columns = slice(p * span, (p + 1) * span)
        pair = recv[pl.ds(2 * last, 2), :, columns].reshape(2 * main, span)
        block = jnp.concatenate([pair, rest_rows[:, columns].astype(jnp.bfloat16)], axis=0)
        piece = times_weight(block, columns)
        product = piece if product is None else product + piece
    scaled, peak_here = finish(product)
    peak = jnp.maximum(peak, peak_here)

    at = lax.broadcasted_iota(jnp.int32, (1, LANES), 1)
    hidden_peak = jnp.where(at == own, peak, 0.0)
    part = lax.broadcasted_iota(jnp.int32, (8, LANES), 0)
    mine[...] = jnp.where(part == 0, grad_peak, jnp.where(part == 1, hidden_peak, 0.0))

    def peak_copy(peer, slot, j):
        return pltpu.make_async_remote_copy(
            src_ref=mine, dst_ref=peaks_in.at[slot],
            send_sem=peak_send_sem.at[j], recv_sem=peak_recv_sem.at[slot],
            device_id=(peer // n_exp, peer % n_exp), device_id_type=MESH,
        )

    def peak_start(j, x):
        peak_copy((here + j) % everyone, here, j).start()
        return x

    def peak_fold(j, best):
        peer = (here + j) % everyone
        peak_copy(peer, peer, j).wait_recv()
        return jnp.maximum(best, peaks_in[peer])

    def peak_finish(j, x):
        peak_copy((here + j) % everyone, here, j).wait_send()
        return x

    lax.fori_loop(1, everyone, peak_start, 0)
    put_pair(last, scaled)
    for s in range(n_exp):
        at_row = 2 * main + s * rest
        base = s * capacity
        out_ref[base:base + main, :] = held[s]
        out_ref[base + main:base + capacity, :] = scaled[at_row:at_row + rest].astype(jnp.bfloat16)
    best = lax.fori_loop(1, everyone, peak_fold, mine[...])
    lax.fori_loop(1, everyone, peak_finish, 0)

    best_ref[...] = best

    def drain(j, x):
        for p in range(PARTS):
            outgoing((me + j) % n_exp, p).wait_send()
        outgoing_rest((me + j) % n_exp).wait_send()
        return x

    lax.fori_loop(1, n_exp, drain, 0)


def finish_kernel(hist_g_ref, hist_h_ref, best_ref, out_ref, new_g_ref, new_h_ref, final_ref):
    final_ref[...] = out_ref[...]
    keep = hist_g_ref.shape[0] - 1
    experts = hist_g_ref.shape[1]
    new_g_ref[0:keep, :] = hist_g_ref[1:keep + 1, :]
    new_g_ref[keep:keep + 1, :] = best_ref[0:1, 0:experts]
    new_h_ref[0:keep, :] = hist_h_ref[1:keep + 1, :]
    new_h_ref[keep:keep + 1, :] = best_ref[1:2, 0:experts]


def per_device(grad_out, expert_ids, down_weight, history_grad, history_hidden):
    tokens, width = grad_out.shape
    experts = history_grad.shape[1]
    n_dp, n_exp = lax.axis_size("dp"), lax.axis_size("expert")
    capacity = tokens * 9 // 32
    main = (capacity - 1) // 16 * 16
    rest = capacity - main
    units = down_weight.shape[1]
    vmem = pl.BlockSpec(memory_space=pltpu.VMEM)
    dma = pltpu.SemaphoreType.DMA
    out, best = pl.pallas_call(
        functools.partial(kernel, n_dp, n_exp, experts, capacity),
        out_shape=(
            jax.ShapeDtypeStruct((n_exp * capacity, units), jnp.bfloat16),
            jax.ShapeDtypeStruct((8, LANES), jnp.float32),
        ),
        in_specs=[pl.BlockSpec(memory_space=pl.ANY), vmem, vmem, vmem, pl.BlockSpec(memory_space=pl.ANY)],
        out_specs=(vmem, vmem),
        scratch_shapes=[
            pltpu.VMEM((tokens, width), jnp.bfloat16),
            pltpu.VMEM((n_exp, main, units), jnp.bfloat16),
            pltpu.VMEM((units, width), jnp.bfloat16),
            pltpu.VMEM((experts, main, width), jnp.bfloat16),
            pltpu.VMEM((experts, rest, width), jnp.bfloat16),
            pltpu.VMEM((n_exp, main, width), jnp.bfloat16),
            pltpu.VMEM((n_exp, rest, width), jnp.bfloat16),
            pltpu.VMEM((n_exp * rest, width), jnp.float32),
            pltpu.VMEM((LANES, tokens), jnp.float32),
            pltpu.VMEM((8, LANES), jnp.float32),
            pltpu.VMEM((n_dp * n_exp, 8, LANES), jnp.float32),
            dma, dma, dma((PARTS, n_exp)), dma((PARTS, n_exp)), dma((n_exp,)), dma((n_exp,)),
            dma((n_dp * n_exp,)), dma((n_dp * n_exp,)),
        ],
        compiler_params=pltpu.CompilerParams(
            collective_id=0, has_side_effects=True, vmem_limit_bytes=60 * 1024 * 1024
        ),
    )(grad_out, expert_ids.T, history_grad, history_hidden, down_weight)
    new_g, new_h, out = pl.pallas_call(
        finish_kernel,
        out_shape=(
            jax.ShapeDtypeStruct(history_grad.shape, jnp.float32),
            jax.ShapeDtypeStruct(history_hidden.shape, jnp.float32),
            jax.ShapeDtypeStruct(out.shape, out.dtype),
        ),
        in_specs=[vmem, vmem, vmem, vmem],
        out_specs=(vmem, vmem, vmem),
    )(history_grad, history_hidden, best, out)
    return out.reshape(1, 1, n_exp * capacity, units), new_g, new_h


def solution(mesh):
    in_specs = (
        P(("dp", "expert"), None),
        P(("dp", "expert"), None),
        P("expert", None, None),
        P(),
        P(),
    )
    out_specs = (P("dp", "expert", None, None), P(), P())
    return jax.shard_map(
        per_device, mesh=mesh, in_specs=in_specs, out_specs=out_specs, check_vma=False
    )
```

```python
import functools

import jax
import jax.numpy as jnp
from jax import lax
from jax.experimental import pallas as pl
from jax.experimental.pallas import tpu as pltpu
from jax.sharding import PartitionSpec as P

MESH = pl.DeviceIdType.MESH
PARTS = 6
LANES = 128


def flip_bits(q, k, count):
    out, bit = 0, 1
    while bit < count:
        a, b = (q // bit) % 2, (k // bit) % 2
        out = out + bit * (a + b - 2 * a * b)
        bit *= 2
    return out


def kernel(
    n_dp, n_exp, experts, capacity,
    grad_hbm, ids_ref, hist_g_ref, hist_h_ref, weight_hbm,
    out_ref, best_ref,
    grad_ref, held, weight, send, send_rest, recv, recv_rest, rest_rows, slots, mine, peaks_in,
    grad_sem, weight_sem, send_sem, recv_sem, send_rest_sem, recv_rest_sem, peak_send_sem, peak_recv_sem,
):
    tokens = grad_ref.shape[0]
    main = send.shape[1]
    slices = n_exp // experts
    chips = n_exp // 2
    my_dp, me = lax.axis_index("dp"), lax.axis_index("expert")
    q0, c0 = me // 2, me % 2
    partner = q0 * 2 + 1 - c0
    own = me // slices
    grad_load = pltpu.make_async_copy(grad_hbm, grad_ref, grad_sem)
    grad_load.start()
    load = pltpu.make_async_copy(weight_hbm.at[0], weight, weight_sem)

    barrier = pltpu.get_barrier_semaphore()

    everyone = n_dp * n_exp
    here = my_dp * n_exp + me

    def greet(j, x):
        peer = (here + j) % everyone
        pl.semaphore_signal(
            barrier, inc=1, device_id=(peer // n_exp, peer % n_exp), device_id_type=MESH
        )
        return x

    lax.fori_loop(1, everyone, greet, 0)

    expert_row = lax.broadcasted_iota(jnp.int32, (LANES, tokens), 0)
    ids = ids_ref[...]
    mask_t = jnp.where((ids[0:1, :] == expert_row) | (ids[1:2, :] == expert_row), 1.0, 0.0)
    row = lax.broadcasted_iota(jnp.int32, (tokens, tokens), 0)
    col = lax.broadcasted_iota(jnp.int32, (tokens, tokens), 1)
    earlier = jnp.where(row < col, 1.0, 0.0).astype(jnp.bfloat16)
    before = jnp.dot(mask_t.astype(jnp.bfloat16), earlier, preferred_element_type=jnp.float32)
    slots[...] = jnp.where(mask_t > 0.5, before, -1.0)
    scale_in = 1.0 / jnp.max(hist_g_ref[...], axis=0, keepdims=True)
    scale_hidden = 1.0 / jnp.max(hist_h_ref[...], axis=0, keepdims=True)
    which = lax.broadcasted_iota(jnp.int32, (1, experts), 1)

    def pick(values, e):
        return jnp.sum(jnp.where(which == e, values, 0.0), axis=1, keepdims=True)

    position = lax.broadcasted_iota(jnp.int32, (capacity, tokens), 0).astype(jnp.float32)

    def prepare(e):
        onehot = jnp.where(slots[pl.ds(e, 1), :] == position, 1.0, 0.0).astype(jnp.bfloat16)
        rows = jnp.dot(onehot, grad_ref[...], preferred_element_type=jnp.float32)
        block = jnp.clip(rows * pick(scale_in, e), -1.0, 1.0)
        send[e] = block[0:main].astype(jnp.bfloat16)
        send_rest[e] = block[main:capacity].astype(jnp.bfloat16)

    span = weight.shape[1] // PARTS

    def outgoing(d, p):
        columns = pl.ds(p * span, span)
        return pltpu.make_async_remote_copy(
            src_ref=send.at[d // slices, :, columns], dst_ref=recv.at[me, :, columns],
            send_sem=send_sem.at[p, d], recv_sem=recv_sem.at[p, me],
            device_id=(my_dp, d), device_id_type=MESH,
        )

    def outgoing_rest(d):
        return pltpu.make_async_remote_copy(
            src_ref=send_rest.at[d // slices], dst_ref=recv_rest.at[me],
            send_sem=send_rest_sem.at[d], recv_sem=recv_rest_sem.at[me],
            device_id=(my_dp, d), device_id_type=MESH,
        )

    def incoming(s, p):
        columns = pl.ds(p * span, span)
        return pltpu.make_async_remote_copy(
            src_ref=send.at[0, :, columns], dst_ref=recv.at[s, :, columns],
            send_sem=send_sem.at[p, s], recv_sem=recv_sem.at[p, s],
            device_id=(my_dp, s), device_id_type=MESH,
        )

    def incoming_rest(s):
        return pltpu.make_async_remote_copy(
            src_ref=send_rest.at[0], dst_ref=recv_rest.at[s],
            send_sem=send_rest_sem.at[s], recv_sem=recv_rest_sem.at[s],
            device_id=(my_dp, s), device_id_type=MESH,
        )

    def chip_of(j):
        k = j
        if chips & (chips - 1) == 0:
            return flip_bits(q0, k, chips)
        return (q0 + k) % chips

    def source_of(j):
        if chips & (chips - 1) == 0:
            return chip_of(j)
        k = j
        return (q0 + chips - k) % chips

    def prepare_pair(q):
        prepare(2 * q + c0)
        prepare(2 * q + 1 - c0)

    def send_pair(q):
        for p in range(PARTS):
            for c in (c0, 1 - c0):
                outgoing(2 * q + c, p).start()
                if p == 0:
                    outgoing_rest(2 * q + c).start()

    greeted = everyone - 1
    grad_load.wait()
    load.start()
    if slices == 1:
        prepare_pair(chip_of(jnp.int32(1)))
        pl.semaphore_wait(barrier, greeted)

        def step(j, x):
            prepare_pair(chip_of((j + 1) % chips))
            send_pair(chip_of(j))
            return x
    else:
        def fill(e, x):
            prepare(e)
            return x

        lax.fori_loop(0, experts, fill, 0)
        pl.semaphore_wait(barrier, greeted)

        def step(j, x):
            send_pair(chip_of(j))
            return x

    lax.fori_loop(1, chips, step, 0)
    for p in range(PARTS):
        outgoing(partner, p).start()
    outgoing_rest(partner).start()

    recv[me] = send[own]
    recv_rest[me] = send_rest[own]
    row_peak = jnp.max(jnp.abs(grad_ref[...]).astype(jnp.float32), axis=1, keepdims=True)
    grad_peak = jnp.max(jnp.where(mask_t.T > 0.5, row_peak, 0.0), axis=0, keepdims=True)

    back = 1.0 / pick(scale_in, own)
    own_hidden = pick(scale_hidden, own)
    load.wait()

    def times_weight(block, columns):
        return lax.dot_general(
            block, weight[:, columns], (((1,), (1,)), ((), ())), preferred_element_type=jnp.float32
        )

    def multiply(block):
        return finish(times_weight(block, slice(None)))

    def finish(product):
        hidden = product * back
        scaled = jnp.clip(hidden * own_hidden, -1.0, 1.0)
        return scaled, jnp.max(jnp.max(jnp.abs(hidden), axis=0, keepdims=True), axis=1, keepdims=True)

    def pair_rows(q):
        return recv[pl.ds(2 * q, 2)].reshape(2 * main, recv.shape[2])

    def put_pair(q, scaled):
        for c in range(2):
            held[2 * q + c] = scaled[c * main:(c + 1) * main].astype(jnp.bfloat16)

    def take_own():
        for p in range(PARTS):
            incoming(partner, p).wait_recv()
        scaled, peak = multiply(pair_rows(q0))
        put_pair(q0, scaled)
        return peak

    def take(j, peak):
        q = source_of(j)
        for p in range(PARTS):
            incoming(2 * q, p).wait_recv()
            incoming(2 * q + 1, p).wait_recv()
        scaled, peak_here = multiply(pair_rows(q))
        put_pair(q, scaled)
        return jnp.maximum(peak, peak_here)

    peak = lax.fori_loop(1, chips - 1, take, take_own())

    def take_rest(j, x):
        incoming_rest((me + j) % n_exp).wait_recv()
        return x

    lax.fori_loop(1, n_exp, take_rest, 0)
    rest = capacity - main
    for s in range(n_exp):
        rest_rows[s * rest:(s + 1) * rest, :] = recv_rest[s].astype(jnp.float32)
    last = source_of(jnp.int32(chips - 1))
    product = None
    for p in range(PARTS):
        incoming(2 * last, p).wait_recv()
        incoming(2 * last + 1, p).wait_recv()
        columns = slice(p * span, (p + 1) * span)
        pair = recv[pl.ds(2 * last, 2), :, columns].reshape(2 * main, span)
        block = jnp.concatenate([pair, rest_rows[:, columns].astype(jnp.bfloat16)], axis=0)
        piece = times_weight(block, columns)
        product = piece if product is None else product + piece
    scaled, peak_here = finish(product)
    peak = jnp.maximum(peak, peak_here)

    at = lax.broadcasted_iota(jnp.int32, (1, LANES), 1)
    hidden_peak = jnp.where(at == own, peak, 0.0)
    part = lax.broadcasted_iota(jnp.int32, (8, LANES), 0)
    mine[...] = jnp.where(part == 0, grad_peak, jnp.where(part == 1, hidden_peak, 0.0))

    def peak_copy(peer, slot, j):
        return pltpu.make_async_remote_copy(
            src_ref=mine, dst_ref=peaks_in.at[slot],
            send_sem=peak_send_sem.at[j], recv_sem=peak_recv_sem.at[slot],
            device_id=(peer // n_exp, peer % n_exp), device_id_type=MESH,
        )

    def peak_start(j, x):
        peak_copy((here + j) % everyone, here, j).start()
        return x

    def peak_fold(j, best):
        peer = (here + j) % everyone
        peak_copy(peer, peer, j).wait_recv()
        return jnp.maximum(best, peaks_in[peer])

    def peak_finish(j, x):
        peak_copy((here + j) % everyone, here, j).wait_send()
        return x

    lax.fori_loop(1, everyone, peak_start, 0)
    put_pair(last, scaled)
    for s in range(n_exp):
        at_row = 2 * main + s * rest
        base = s * capacity
        out_ref[base:base + main, :] = held[s]
        out_ref[base + main:base + capacity, :] = scaled[at_row:at_row + rest].astype(jnp.bfloat16)
    best = lax.fori_loop(1, everyone, peak_fold, mine[...])
    lax.fori_loop(1, everyone, peak_finish, 0)

    best_ref[...] = best

    def drain(j, x):
        for p in range(PARTS):
            outgoing((me + j) % n_exp, p).wait_send()
        outgoing_rest((me + j) % n_exp).wait_send()
        return x

    lax.fori_loop(1, n_exp, drain, 0)


def finish_kernel(hist_g_ref, hist_h_ref, best_ref, out_ref, new_g_ref, new_h_ref, final_ref):
    final_ref[...] = out_ref[...]
    keep = hist_g_ref.shape[0] - 1
    experts = hist_g_ref.shape[1]
    new_g_ref[0:keep, :] = hist_g_ref[1:keep + 1, :]
    new_g_ref[keep:keep + 1, :] = best_ref[0:1, 0:experts]
    new_h_ref[0:keep, :] = hist_h_ref[1:keep + 1, :]
    new_h_ref[keep:keep + 1, :] = best_ref[1:2, 0:experts]


def per_device(grad_out, expert_ids, down_weight, history_grad, history_hidden):
    tokens, width = grad_out.shape
    experts = history_grad.shape[1]
    n_dp, n_exp = lax.axis_size("dp"), lax.axis_size("expert")
    capacity = tokens * 9 // 32
    main = (capacity - 1) // 16 * 16
    rest = capacity - main
    units = down_weight.shape[1]
    vmem = pl.BlockSpec(memory_space=pltpu.VMEM)
    dma = pltpu.SemaphoreType.DMA
    out, best = pl.pallas_call(
        functools.partial(kernel, n_dp, n_exp, experts, capacity),
        out_shape=(
            jax.ShapeDtypeStruct((n_exp * capacity, units), jnp.bfloat16),
            jax.ShapeDtypeStruct((8, LANES), jnp.float32),
        ),
        in_specs=[pl.BlockSpec(memory_space=pl.ANY), vmem, vmem, vmem, pl.BlockSpec(memory_space=pl.ANY)],
        out_specs=(vmem, vmem),
        scratch_shapes=[
            pltpu.VMEM((tokens, width), jnp.bfloat16),
            pltpu.VMEM((n_exp, main, units), jnp.bfloat16),
            pltpu.VMEM((units, width), jnp.bfloat16),
            pltpu.VMEM((experts, main, width), jnp.bfloat16),
            pltpu.VMEM((experts, rest, width), jnp.bfloat16),
            pltpu.VMEM((n_exp, main, width), jnp.bfloat16),
            pltpu.VMEM((n_exp, rest, width), jnp.bfloat16),
            pltpu.VMEM((n_exp * rest, width), jnp.float32),
            pltpu.VMEM((LANES, tokens), jnp.float32),
            pltpu.VMEM((8, LANES), jnp.float32),
            pltpu.VMEM((n_dp * n_exp, 8, LANES), jnp.float32),
            dma, dma, dma((PARTS, n_exp)), dma((PARTS, n_exp)), dma((n_exp,)), dma((n_exp,)),
            dma((n_dp * n_exp,)), dma((n_dp * n_exp,)),
        ],
        compiler_params=pltpu.CompilerParams(
            collective_id=0, has_side_effects=True, vmem_limit_bytes=60 * 1024 * 1024
        ),
    )(grad_out, expert_ids.T, history_grad, history_hidden, down_weight)
    new_g, new_h, out = pl.pallas_call(
        finish_kernel,
        out_shape=(
            jax.ShapeDtypeStruct(history_grad.shape, jnp.float32),
            jax.ShapeDtypeStruct(history_hidden.shape, jnp.float32),
            jax.ShapeDtypeStruct(out.shape, out.dtype),
        ),
        in_specs=[vmem, vmem, vmem, vmem],
        out_specs=(vmem, vmem, vmem),
    )(history_grad, history_hidden, best, out)
    return out.reshape(1, 1, n_exp * capacity, units), new_g, new_h


def solution(mesh):
    in_specs = (
        P(("dp", "expert"), None),
        P(("dp", "expert"), None),
        P("expert", None, None),
        P(),
        P(),
    )
    out_specs = (P("dp", "expert", None, None), P(), P())
    return jax.shard_map(
        per_device, mesh=mesh, in_specs=in_specs, out_specs=out_specs, check_vma=False
    )
```
